32 devices in a mesh: cell: 16 (over z, y, x), gene: 2 (over core).
Axes of the slice: x: 2, y: 2, z: 4, core: 2. Of those that a mesh axis runs over, the one named last changes fastest.
Arguments:
- tiles: bfloat16 [2, 1024, 128, 128], P('gene', 'cell'), may hold values from -8 to 8
- tile_row: int32 [2, 1024], P('gene', 'cell'), may hold values from 0 to 7, as said below
- tile_col: int32 [2, 1024], P('gene', 'cell'), may hold values from 0 to 15
- tile_count: int32 [2, 16], P('gene', 'cell'), may hold values from 1 to 64, as said below
- start_basis: bfloat16 [64, 4096], P(None, 'gene'), may hold values from -0.09375 to 0.09375
Outputs:
- basis: bfloat16 [64, 16384], P(None, 'cell')
- loadings: float32 [64, 4096], P(None, ('gene', 'cell'))
The draws below stay inside these ranges and needn't reach their ends.
Inputs may be any that keep to these rules, and one draw needn't show every extreme that they name: `tile_row`: tile row of each slot, within 0 to 7; the slots of one device name distinct (row, column) pairs. `tile_count`: slots in use; for each index of gene some device uses all 64.
All inputs are finite; a program needn't handle non-finite values.
Results may differ from the reference program's by a relative error of at most 0.018.
Values may be sent and summed in bfloat16 or wider, within the bound.
A program may use at most 64 MiB of HBM per device.

```python
import jax
import jax.numpy as jnp
from jax import lax

K = 64
G = 4096
TILE = 128
ROW_BLOCKS = 8
N_CELL = 16
N_GENE = 2


strongest = 32.0


tile_scale = 0.125


def slot_places(key):
    base = jax.random.fold_in(key, 7)
    gene_blocks = G // (N_GENE * TILE)
    slot_count = ROW_BLOCKS * gene_blocks // 2
    keys = jax.random.split(base, N_GENE * N_CELL)

    def one_device(device_key):
        return jax.random.permutation(device_key, ROW_BLOCKS * gene_blocks)[:slot_count].astype(jnp.int32)
    places = jax.vmap(one_device)(keys)
    return (places.reshape(N_GENE, N_CELL * slot_count), gene_blocks)


def draw_tiles(key, part):
    places, gene_blocks = slot_places(key)
    slot_count = ROW_BLOCKS * gene_blocks // 2
    columns_all = G // TILE
    per_column = (K + columns_all - 1) // columns_all
    row_local = places // gene_blocks
    col_local = places % gene_blocks
    gene_of = jnp.arange(N_GENE, dtype=jnp.int32)[:, None]
    cell_of = (jnp.arange(N_CELL * slot_count, dtype=jnp.int32) // slot_count)[None, :]
    global_col = (gene_of * gene_blocks + col_local).reshape(N_GENE * N_CELL, slot_count).astype(jnp.int32)
    global_row = (cell_of * ROW_BLOCKS + row_local).reshape(N_GENE * N_CELL, slot_count).astype(jnp.int32)
    ladder = strongest ** (jnp.arange(K, dtype=jnp.float32) / jnp.float32(K - 1))
    order = jax.random.permutation(jax.random.fold_in(key, 21), K)
    strength = ladder[order]
    component = jnp.arange(columns_all, dtype=jnp.int32)[:, None] + columns_all * jnp.arange(per_column, dtype=jnp.int32)[None, :]
    column_strength = jnp.where(component < K, strength[jnp.minimum(component, K - 1)], 0.0)
    gene_factor = jax.random.truncated_normal(jax.random.fold_in(key, 23), -3.0, 3.0, (columns_all, per_column, TILE), jnp.float32)
    gene_factor = gene_factor / jnp.sqrt(jnp.float32(TILE))
    cell_key = jax.random.fold_in(key, 27)
    noise_key = jax.random.fold_in(key, 25)
    rise_ratio = 3.0

    def one_device(index):
        columns = global_col[index]
        rows = global_row[index]
        cell_index = (index % N_CELL).astype(jnp.float32)
        rise = jnp.float32(rise_ratio) ** (cell_index / jnp.float32(max(N_CELL - 1, 1)))
        slot_keys = jax.vmap(lambda row, col: jax.random.fold_in(cell_key, row * columns_all + col))(rows, columns)
        device_key = jax.random.fold_in(noise_key, index)
        cell_factor = jax.vmap(lambda one_key: jax.random.truncated_normal(one_key, -3.0, 3.0, (per_column, TILE), jnp.float32))(slot_keys)
        noise = jax.random.truncated_normal(device_key, -4.0, 4.0, (slot_count, TILE, TILE), jnp.float32)
        weighted = cell_factor * column_strength[columns][:, :, None]
        planted = jnp.einsum('spr,spg->srg', weighted, gene_factor[columns])
        return jnp.clip(tile_scale * rise * (noise + planted), -8.0, 8.0).astype(jnp.bfloat16)
    stacked = lax.map(one_device, jnp.arange(N_GENE * N_CELL, dtype=jnp.int32))
    return stacked.reshape(N_GENE, N_CELL * slot_count, TILE, TILE)


def draw_tile_row(key, part):
    places, gene_blocks = slot_places(key)
    return (places // gene_blocks).astype(jnp.int32)


def draw_tile_col(key, part):
    places, gene_blocks = slot_places(key)
    return (places % gene_blocks).astype(jnp.int32)


def draw_tile_count(key, part):
    slot_count = ROW_BLOCKS * (G // (N_GENE * TILE)) // 2
    first_key, second_key = jax.random.split(jax.random.fold_in(key, 11))
    lowest = max(1, slot_count // 8)
    highest = max(lowest + 1, slot_count * 7 // 8 + 1)
    counts = jax.random.randint(first_key, (N_GENE, N_CELL), lowest, highest, dtype=jnp.int32)
    fullest = jax.random.randint(second_key, (N_GENE, 1), 0, N_CELL, dtype=jnp.int32)
    return jnp.where(jnp.arange(N_CELL, dtype=jnp.int32)[None, :] == fullest, slot_count, counts).astype(jnp.int32)


def block_scale(key, shape, pieces, least, high):
    gain = 1.0
    for dim, blocks in pieces:
        steps = jax.random.uniform(jax.random.fold_in(jax.random.fold_in(key, 6), dim), (blocks,), jnp.float32, least / len(pieces), high / len(pieces))
        gain = gain * jnp.repeat(jnp.exp(steps), shape[dim] // blocks).reshape((-1,) + (1,) * (len(shape) - 1 - dim))
    return gain


def scatter_about(key, extent, width, bound, cuts=(), kind=jnp.bfloat16):
    values = jax.random.normal(key, extent, jnp.float32) * width
    if len(cuts) > 0:
        values = block_scale(key, extent, cuts, -0.22, 0.18) * values
    return jnp.clip(values, min=-bound, max=bound).astype(kind)


def setup_inputs(seed: int = 0) -> dict:
    key_list = jax.random.split(jax.random.key(seed), 6)
    tiles = draw_tiles(jax.random.fold_in(key_list[5], 71), 0)
    tile_row = draw_tile_row(jax.random.fold_in(key_list[5], 71), 0)
    tile_col = draw_tile_col(jax.random.fold_in(key_list[5], 71), 0)
    tile_count = draw_tile_count(jax.random.fold_in(key_list[5], 71), 0)
    start_basis = scatter_about(key_list[4], (K, G), G ** -0.5, 0.09375, ((1, 2),))
    return {"tiles": tiles, "tile_row": tile_row, "tile_col": tile_col, "tile_count": tile_count, "start_basis": start_basis}


def solve_lower(lower, right):
    return lax.linalg.triangular_solve(lower, right, left_side=True, lower=True)

def gram_of(scores):
    return jnp.dot(scores.astype(jnp.float32), scores.T.astype(jnp.float32), precision=lax.Precision.HIGHEST, preferred_element_type=jnp.float32)

def orthonormal(scores):
    lower_one = jnp.linalg.cholesky(gram_of(scores))
    return solve_lower(lower_one, scores)

def reference(tiles, tile_row, tile_col, tile_count, start_basis):
    slot_count = tiles.shape[1] // N_CELL
    gene_dev = G // N_GENE
    gene_blocks = gene_dev // TILE
    cell_dev = ROW_BLOCKS * TILE
    grouped = tiles.reshape(N_GENE, N_CELL, slot_count, TILE, TILE)
    rows_all = tile_row.reshape(N_GENE, N_CELL, slot_count)
    cols_all = tile_col.reshape(N_GENE, N_CELL, slot_count)

    def onehots(gene, cell):
        live_mask = (jnp.arange(slot_count) < tile_count[gene, cell]).astype(jnp.float32)
        row_hot = (rows_all[gene, cell][:, None] == jnp.arange(ROW_BLOCKS)[None, :]).astype(jnp.float32) * live_mask[:, None]
        col_hot = (cols_all[gene, cell][:, None] == jnp.arange(gene_blocks)[None, :]).astype(jnp.float32) * live_mask[:, None]
        return (row_hot, col_hot)

    def scores_of(basis):

        def one_cell(cell):
            total = jnp.zeros((K, cell_dev), jnp.float32)
            for gene in range(N_GENE):
                row_hot, col_hot = onehots(gene, cell)
                local = basis[:, gene * gene_dev:(gene + 1) * gene_dev].reshape(K, gene_blocks, TILE)
                picked = jnp.take(local, cols_all[gene, cell], axis=1).astype(jnp.float32)
                products = jnp.einsum('ksg,srg->skr', picked, grouped[gene, cell].astype(jnp.float32), precision=lax.Precision.HIGHEST)
                summed = jnp.einsum('sb,skr->kbr', row_hot, products, precision=lax.Precision.HIGHEST)
                total = total + summed.reshape(K, cell_dev)
            return total
        stacked = lax.map(one_cell, jnp.arange(N_CELL))
        return jnp.transpose(stacked, (1, 0, 2)).reshape(K, N_CELL * cell_dev)

    def loadings_of(ortho_half):
        blocks = ortho_half.reshape(K, N_CELL, cell_dev)

        def step(carry, cell):
            parts = []
            for gene in range(N_GENE):
                row_hot, col_hot = onehots(gene, cell)
                local = blocks[:, cell].reshape(K, ROW_BLOCKS, TILE)
                picked = jnp.take(local, rows_all[gene, cell], axis=1).astype(jnp.float32)
                products = jnp.einsum('ksr,srg->skg', picked, grouped[gene, cell].astype(jnp.float32), precision=lax.Precision.HIGHEST)
                summed = jnp.einsum('sb,skg->kbg', col_hot, products, precision=lax.Precision.HIGHEST)
                parts.append(summed.reshape(K, gene_dev))
            return (carry + jnp.stack(parts), None)
        start = jnp.zeros((N_GENE, K, gene_dev), jnp.float32)
        total, _ = lax.scan(step, start, jnp.arange(N_CELL))
        return jnp.transpose(total, (1, 0, 2)).reshape(K, G)
    ortho = orthonormal(scores_of(start_basis))
    middle = loadings_of(ortho.astype(jnp.bfloat16))
    ortho_two = orthonormal(scores_of(middle.astype(jnp.bfloat16)))
    loadings = loadings_of(ortho_two.astype(jnp.bfloat16))
    basis = (ortho_two * jnp.sqrt(jnp.float32(N_CELL * cell_dev))).astype(jnp.bfloat16)
    return (basis, loadings)
```

```python
import functools

import jax
import jax.numpy as jnp
from jax import lax
from jax.experimental import pallas as pl
from jax.experimental.pallas import tpu as pltpu
from jax.sharding import PartitionSpec as P

ROW_BLOCKS = 8
PANEL = 4
MESH = pl.DeviceIdType.MESH
HIGH = lax.Precision.HIGHEST


def split_three(value):
    high = value.astype(jnp.bfloat16)
    rest = value - high.astype(jnp.float32)
    middle = rest.astype(jnp.bfloat16)
    low = (rest - middle.astype(jnp.float32)).astype(jnp.bfloat16)
    return high, middle, low


def inverse_factor(gram):
    width = gram.shape[0]
    shape = (width, 2 * width)
    row = lax.broadcasted_iota(jnp.int32, shape, 0)
    lane = lax.broadcasted_iota(jnp.int32, shape, 1)
    both = jnp.concatenate([jnp.zeros_like(gram), gram], axis=1)
    both = jnp.where(row == lane, 1.0, both)
    pivots = jnp.ones(shape, jnp.float32)
    done = []
    start = 0
    for first in range(0, width, PANEL):
        base = first // 8 * 8
        if base > start:
            done.append((both[: base - start], pivots[: base - start]))
            both = both[base - start :]
            pivots = pivots[base - start :]
            row = row[base - start :]
            start = base
        columns = [
            jnp.broadcast_to(both[:, width + j : width + j + 1], both.shape)
            for j in range(first, first + PANEL)
        ]
        for k in range(PANEL):
            j = first + k
            at = j - start
            pivot = columns[k][at : at + 1]
            factor = jnp.where(row > j, columns[k] * (1.0 / pivot), 0.0)
            pivots = jnp.where(row == j, pivot, pivots)
            both = both - factor * both[at : at + 1]
            for m in range(k + 1, PANEL):
                columns[m] = columns[m] - factor * columns[m][at : at + 1]
    done.append((both, pivots))
    both = jnp.concatenate([piece for piece, _ in done], axis=0)
    pivots = jnp.concatenate([piece for _, piece in done], axis=0)
    return (both * lax.rsqrt(pivots))[:, :width]


def kernel(
    cells, genes, parts,
    table, tiles, start, basis_out, load_out,
    held, dense, mine, theirs, stacked, grams, sums_out, sums_in, middle,
    tile_sem, pair_send, pair_recv, gram_send, gram_recv,
    sum_send, sum_recv, mid_send, mid_recv,
):
    cell = lax.axis_index("cell")
    gene = lax.axis_index("gene")
    slots, side, _ = tiles.shape
    width = start.shape[0]
    cell_dev, gene_dev = dense.shape
    gene_blocks = gene_dev // side
    chunk = gene_dev // cells
    piece = cell_dev // parts
    half = width // 2
    other = lax.rem(gene + 1, genes)

    fetch = pltpu.make_async_copy(tiles, held.at[pl.ds(0, slots)], tile_sem)
    fetch.start()

    barrier = pltpu.get_barrier_semaphore()

    def greet(k, _):
        pl.semaphore_signal(
            barrier, inc=1, device_id={"cell": lax.rem(cell + k, cells)}, device_id_type=MESH
        )
        return 0

    pl.semaphore_signal(barrier, inc=1, device_id={"gene": other}, device_id_type=MESH)
    lax.fori_loop(1, cells, greet, 0)
    held[slots] = jnp.zeros((side, side), held.dtype)
    fetch.wait()

    def place(i, _):
        row = i // gene_blocks
        col = lax.rem(i, gene_blocks)
        dense[
            pl.ds(pl.multiple_of(row * side, side), side),
            pl.ds(pl.multiple_of(col * side, side), side),
        ] = held[table[i]]
        return 0

    lax.fori_loop(0, (cell_dev // side) * gene_blocks, place, 0)
    pl.semaphore_wait(barrier, cells)

    def pair_copy(it, r):
        return pltpu.make_async_remote_copy(
            src_ref=mine.at[it, r], dst_ref=theirs.at[it, r],
            send_sem=pair_send.at[it, r], recv_sem=pair_recv.at[it, r],
            device_id={"gene": other}, device_id_type=MESH,
        )

    def gram_copy(it, source, k):
        return pltpu.make_async_remote_copy(
            src_ref=grams.at[it, source], dst_ref=grams.at[it, source],
            send_sem=gram_send.at[it, k], recv_sem=gram_recv.at[it, source],
            device_id={"cell": lax.rem(cell + k, cells)}, device_id_type=MESH,
        )

    def sum_copy(it, source, k):
        target = lax.rem(cell + k, cells)
        return pltpu.make_async_remote_copy(
            src_ref=sums_out.at[it, target], dst_ref=sums_in.at[it, source],
            send_sem=sum_send.at[it, k], recv_sem=sum_recv.at[it, source],
            device_id={"cell": target}, device_id_type=MESH,
        )

    def mid_copy(source, k):
        return pltpu.make_async_remote_copy(
            src_ref=middle.at[source], dst_ref=middle.at[source],
            send_sem=mid_send.at[k], recv_sem=mid_recv.at[source],
            device_id={"cell": lax.rem(cell + k, cells)}, device_id_type=MESH,
        )

    def each(act):
        def body(k, _):
            act(lax.rem(cell + cells - k, cells), k)
            return 0

        lax.fori_loop(1, cells, body, 0)

    for it in range(2):
        if it == 0:
            basis = start[...]
        else:
            basis = jnp.concatenate([middle[c] for c in range(cells)], axis=1)

        for r in range(parts):
            mine[it, r] = lax.dot_general(
                basis, dense[r * piece : (r + 1) * piece, :], (((1,), (1,)), ((), ())),
                preferred_element_type=jnp.float32,
            )
            pair_copy(it, r).start()
        for r in range(parts):
            pair_copy(it, r).wait_recv()
            where = slice(r * piece, (r + 1) * piece)
            high, mid, low = split_three(mine[it, r] + theirs[it, r])
            stacked[0:width, where] = high
            stacked[width : 2 * width, where] = mid
            stacked[2 * width : 3 * width, where] = low

        whole = stacked[...]
        cross = lax.dot_general(
            whole, whole, (((1,), (1,)), ((), ())), preferred_element_type=jnp.float32
        )
        cross = cross[:width] + cross[width : 2 * width] + cross[2 * width :]
        gram = cross[:, :width] + cross[:, width : 2 * width] + cross[:, 2 * width :]
        grams[it, cell] = jnp.concatenate([gram[:half], gram[half:]], axis=1)
        each(lambda _, k: gram_copy(it, cell, k).start())

        def product(columns):
            pair = jnp.dot(
                stacked[0 : 2 * width, :], columns, preferred_element_type=jnp.float32
            )
            return pair[:width] + pair[width:]

        if chunk % 128 == 0:

            def send(k, _):
                target = lax.rem(cell + k, cells)
                sums_out[it, target] = product(
                    dense[:, pl.ds(pl.multiple_of(target * chunk, chunk), chunk)]
                )
                sum_copy(it, cell, k).start()
                return 0

            lax.fori_loop(1, cells, send, 0)
            sums_in[it, cell] = product(
                dense[:, pl.ds(pl.multiple_of(cell * chunk, chunk), chunk)]
            )
        else:
            for b in range(gene_blocks):
                wide = product(dense[:, b * side : (b + 1) * side])
                for c in range(side // chunk):
                    sums_out[it, b * (side // chunk) + c] = wide[:, c * chunk : (c + 1) * chunk]
            each(lambda _, k: sum_copy(it, cell, k).start())
            sums_in[it, cell] = sums_out[it, cell]

        each(lambda source, k: gram_copy(it, source, k).wait_recv())
        total = grams[it, 0]
        for c in range(1, cells):
            total = total + grams[it, c]
        total = jnp.concatenate([total[:, :width], total[:, width:]], axis=0)
        inverse = inverse_factor(total)

        if it == 1:
            scale = jnp.sqrt(jnp.float32(cells * cell_dev))
            for r in range(parts):
                basis_out[:, r * piece : (r + 1) * piece] = (
                    jnp.dot(
                        inverse, mine[it, r] + theirs[it, r], precision=HIGH,
                        preferred_element_type=jnp.float32,
                    ) * scale
                ).astype(basis_out.dtype)

        each(lambda source, k: sum_copy(it, source, k).wait_recv())
        summed = sums_in[it, 0]
        for c in range(1, cells):
            summed = summed + sums_in[it, c]
        result = jnp.dot(inverse, summed, precision=HIGH, preferred_element_type=jnp.float32)
        if it == 0:
            middle[cell] = result.astype(middle.dtype)
            each(lambda _, k: mid_copy(cell, k).start())
            each(lambda source, k: mid_copy(source, k).wait_recv())
        else:
            load_out[...] = result

    for it in range(2):
        for r in range(parts):
            pair_copy(it, r).wait_send()
        each(lambda _, k: gram_copy(it, cell, k).wait_send())
        each(lambda _, k: sum_copy(it, cell, k).wait_send())
    each(lambda _, k: mid_copy(cell, k).wait_send())


def local(cells, genes, tiles, tile_row, tile_col, tile_count, start_basis):
    slots, side = tiles.shape[1], tiles.shape[-1]
    width, gene_dev = start_basis.shape
    gene_blocks = gene_dev // side
    cell_dev = ROW_BLOCKS * side
    chunk = gene_dev // cells
    parts = 4
    places = ROW_BLOCKS * gene_blocks
    live = jnp.arange(slots) < tile_count[0, 0]
    spot = jnp.where(live, tile_row[0] * gene_blocks + tile_col[0], places)
    table = jnp.min(
        jnp.where(spot[None, :] == jnp.arange(places)[:, None], jnp.arange(slots)[None, :], slots),
        axis=1,
    ).astype(jnp.int32)
    dma = pltpu.SemaphoreType.DMA
    return pl.pallas_call(
        functools.partial(kernel, cells, genes, parts),
        out_shape=(
            jax.ShapeDtypeStruct((width, cell_dev), jnp.bfloat16),
            jax.ShapeDtypeStruct((width, chunk), jnp.float32),
        ),
        in_specs=[
            pl.BlockSpec(memory_space=pltpu.SMEM),
            pl.BlockSpec(memory_space=pl.ANY),
            pl.BlockSpec(memory_space=pltpu.VMEM),
        ],
        out_specs=(
            pl.BlockSpec(memory_space=pltpu.VMEM),
            pl.BlockSpec(memory_space=pltpu.VMEM),
        ),
        scratch_shapes=[
            pltpu.VMEM((slots + 1, side, side), jnp.bfloat16),
            pltpu.VMEM((cell_dev, gene_dev), jnp.bfloat16),
            pltpu.VMEM((2, parts, width, cell_dev // parts), jnp.float32),
            pltpu.VMEM((2, parts, width, cell_dev // parts), jnp.float32),
            pltpu.VMEM((3 * width, cell_dev), jnp.bfloat16),
            pltpu.VMEM((2, cells, width // 2, 2 * width), jnp.float32),
            pltpu.VMEM((2, cells, width, chunk), jnp.float32),
            pltpu.VMEM((2, cells, width, chunk), jnp.float32),
            pltpu.VMEM((cells, width, chunk), jnp.bfloat16),
            dma,
            dma((2, parts)), dma((2, parts)),
            dma((2, cells)), dma((2, cells)),
            dma((2, cells)), dma((2, cells)),
            dma((cells,)), dma((cells,)),
        ],
        compiler_params=pltpu.CompilerParams(
            collective_id=0, has_side_effects=True, vmem_limit_bytes=60 * 1024 * 1024
        ),
    )(table, tiles[0], start_basis)


def solution(mesh):
    return jax.shard_map(
        functools.partial(local, mesh.shape["cell"], mesh.shape["gene"]),
        mesh=mesh,
        in_specs=(
            P("gene", "cell", None, None),
            P("gene", "cell"),
            P("gene", "cell"),
            P("gene", "cell"),
            P(None, "gene"),
        ),
        out_specs=(P(None, "cell"), P(None, ("gene", "cell"))),
        check_vma=False,
    )
```

```python
import functools

import jax
import jax.numpy as jnp
from jax import lax
from jax.experimental import pallas as pl
from jax.experimental.pallas import tpu as pltpu
from jax.sharding import PartitionSpec as P

ROW_BLOCKS = 8
PANEL = 4
MESH = pl.DeviceIdType.MESH
HIGH = lax.Precision.HIGHEST


def split_three(value):
    high = value.astype(jnp.bfloat16)
    rest = value - high.astype(jnp.float32)
    middle = rest.astype(jnp.bfloat16)
    low = (rest - middle.astype(jnp.float32)).astype(jnp.bfloat16)
    return high, middle, low


def inverse_factor(gram):
    width = gram.shape[0]
    shape = (width, 2 * width)
    row = lax.broadcasted_iota(jnp.int32, shape, 0)
    lane = lax.broadcasted_iota(jnp.int32, shape, 1)
    both = jnp.concatenate([jnp.zeros_like(gram), gram], axis=1)
    both = jnp.where(row == lane, 1.0, both)
    pivots = jnp.ones(shape, jnp.float32)
    done = []
    start = 0
    for first in range(0, width, PANEL):
        base = first // 8 * 8
        if base > start:
            done.append((both[: base - start], pivots[: base - start]))
            both = both[base - start :]
            pivots = pivots[base - start :]
            row = row[base - start :]
            start = base
        columns = [
            jnp.broadcast_to(both[:, width + j : width + j + 1], both.shape)
            for j in range(first, first + PANEL)
        ]
        for k in range(PANEL):
            j = first + k
            at = j - start
            pivot = columns[k][at : at + 1]
            factor = jnp.where(row > j, columns[k] * (1.0 / pivot), 0.0)
            pivots = jnp.where(row == j, pivot, pivots)
            both = both - factor * both[at : at + 1]
            for m in range(k + 1, PANEL):
                columns[m] = columns[m] - factor * columns[m][at : at + 1]
    done.append((both, pivots))
    both = jnp.concatenate([piece for piece, _ in done], axis=0)
    pivots = jnp.concatenate([piece for _, piece in done], axis=0)
    return (both * lax.rsqrt(pivots))[:, :width]


def kernel(
    cells, inner, genes, parts,
    table, tiles, start, basis_out, load_out,
    held, dense, mine, theirs, stacked, grams, planes, sums_out, sums_mid, sums_own, sums_in, middle,
    tile_sem, pair_send, pair_recv, gram_send, gram_recv, plane_send, plane_recv,
    near_send, near_recv, far_send, far_recv, mid_send, mid_recv,
):
    cell = lax.axis_index("cell")
    gene = lax.axis_index("gene")
    slots, side, _ = tiles.shape
    width = start.shape[0]
    cell_dev, gene_dev = dense.shape
    gene_blocks = gene_dev // side
    chunk = gene_dev // cells
    piece = cell_dev // parts
    half = width // 2
    outer = cells // inner
    here = cell // inner
    spot = lax.rem(cell, inner)
    other = lax.rem(gene + 1, genes)

    fetch = pltpu.make_async_copy(tiles, held.at[pl.ds(0, slots)], tile_sem)
    fetch.start()

    barrier = pltpu.get_barrier_semaphore()

    def greet(k, _):
        pl.semaphore_signal(
            barrier, inc=1, device_id={"cell": lax.rem(cell + k, cells)}, device_id_type=MESH
        )
        return 0

    pl.semaphore_signal(barrier, inc=1, device_id={"gene": other}, device_id_type=MESH)
    lax.fori_loop(1, cells, greet, 0)
    held[slots] = jnp.zeros((side, side), held.dtype)
    fetch.wait()

    def place(i, _):
        row = i // gene_blocks
        col = lax.rem(i, gene_blocks)
        dense[
            pl.ds(pl.multiple_of(row * side, side), side),
            pl.ds(pl.multiple_of(col * side, side), side),
        ] = held[table[i]]
        return 0

    lax.fori_loop(0, (cell_dev // side) * gene_blocks, place, 0)
    pl.semaphore_wait(barrier, cells)

    def pair_copy(it, r):
        return pltpu.make_async_remote_copy(
            src_ref=mine.at[it, r], dst_ref=theirs.at[it, r],
            send_sem=pair_send.at[it, r], recv_sem=pair_recv.at[it, r],
            device_id={"gene": other}, device_id_type=MESH,
        )

    def near(k):
        return here * inner + lax.rem(spot + k, inner)

    def far(k):
        return lax.rem(here + k, outer) * inner + spot

    def gram_copy(it, source, k):
        return pltpu.make_async_remote_copy(
            src_ref=grams.at[it, source], dst_ref=grams.at[it, source],
            send_sem=gram_send.at[it, k], recv_sem=gram_recv.at[it, source],
            device_id={"cell": near(k)}, device_id_type=MESH,
        )

    def plane_copy(it, source, k):
        return pltpu.make_async_remote_copy(
            src_ref=planes.at[it, source], dst_ref=planes.at[it, source],
            send_sem=plane_send.at[it, k], recv_sem=plane_recv.at[it, source],
            device_id={"cell": far(k)}, device_id_type=MESH,
        )

    def near_copy(it, group, source, k):
        return pltpu.make_async_remote_copy(
            src_ref=sums_out.at[it, group, lax.rem(spot + k, inner)],
            dst_ref=sums_mid.at[it, group, source],
            send_sem=near_send.at[it, group, k], recv_sem=near_recv.at[it, group, source],
            device_id={"cell": near(k)}, device_id_type=MESH,
        )

    def far_copy(it, source, k):
        return pltpu.make_async_remote_copy(
            src_ref=sums_own.at[it, lax.rem(here + k, outer)], dst_ref=sums_in.at[it, source],
            send_sem=far_send.at[it, k], recv_sem=far_recv.at[it, source],
            device_id={"cell": far(k)}, device_id_type=MESH,
        )

    def mid_copy(source, k):
        return pltpu.make_async_remote_copy(
            src_ref=middle.at[source], dst_ref=middle.at[source],
            send_sem=mid_send.at[k], recv_sem=mid_recv.at[source],
            device_id={"cell": lax.rem(cell + k, cells)}, device_id_type=MESH,
        )

    def each(act):
        def body(k, _):
            act(lax.rem(cell + cells - k, cells), k)
            return 0

        lax.fori_loop(1, cells, body, 0)

    def each_near(act):
        for k in range(1, inner):
            act(lax.rem(spot + inner - k, inner), k)

    def each_far(act):
        for k in range(1, outer):
            act(lax.rem(here + outer - k, outer), k)

    def added(ref, count):
        total = ref[0]
        for c in range(1, count):
            total = total + ref[c]
        return total

    for it in range(2):
        if it == 0:
            basis = start[...]
        else:
            basis = jnp.concatenate([middle[c] for c in range(cells)], axis=1)

        for r in range(parts):
            mine[it, r] = lax.dot_general(
                basis, dense[r * piece : (r + 1) * piece, :], (((1,), (1,)), ((), ())),
                preferred_element_type=jnp.float32,
            )
            pair_copy(it, r).start()
        for r in range(parts):
            pair_copy(it, r).wait_recv()
            where = slice(r * piece, (r + 1) * piece)
            high, mid, low = split_three(mine[it, r] + theirs[it, r])
            stacked[0:width, where] = high
            stacked[width : 2 * width, where] = mid
            stacked[2 * width : 3 * width, where] = low

        whole = stacked[...]
        cross = lax.dot_general(
            whole, whole, (((1,), (1,)), ((), ())), preferred_element_type=jnp.float32
        )
        cross = cross[:width] + cross[width : 2 * width] + cross[2 * width :]
        gram = cross[:, :width] + cross[:, width : 2 * width] + cross[:, 2 * width :]
        grams[it, spot] = jnp.concatenate([gram[:half], gram[half:]], axis=1)
        each_near(lambda _, k: gram_copy(it, spot, k).start())

        def product(columns):
            pair = jnp.dot(
                stacked[0 : 2 * width, :], columns, preferred_element_type=jnp.float32
            )
            return pair[:width] + pair[width:]

        span = inner * chunk

        def multiply(k):
            group = lax.rem(here + k, outer)
            if span % 128 == 0:
                wide = product(dense[:, pl.ds(pl.multiple_of(group * span, 128), span)])
                for c in range(inner):
                    sums_out[it, group, c] = wide[:, c * chunk : (c + 1) * chunk]
            each_near(lambda _, k: near_copy(it, group, spot, k).start())

        def forward(k):
            group = lax.rem(here + k, outer)
            each_near(lambda source, k: near_copy(it, group, source, k).wait_recv())
            total = sums_out[it, group, spot]
            for c in range(1, inner):
                total = total + sums_mid[it, group, lax.rem(spot + c, inner)]
            if k == 0:
                sums_in[it, here] = total
            else:
                sums_own[it, group] = total
                far_copy(it, here, k).start()

        if span % 128 != 0:
            for b in range(gene_blocks):
                wide = product(dense[:, b * side : (b + 1) * side])
                for c in range(side // chunk):
                    at = b * (side // chunk) + c
                    sums_out[it, at // inner, at % inner] = wide[:, c * chunk : (c + 1) * chunk]
        multiply(1)
        each_near(lambda source, k: gram_copy(it, source, k).wait_recv())
        planes[it, here] = added(grams.at[it], inner)
        each_far(lambda _, k: plane_copy(it, here, k).start())
        for k in range(2, outer):
            multiply(k)
        multiply(0)
        for k in range(1, outer):
            forward(k)
        each_far(lambda source, k: plane_copy(it, source, k).wait_recv())
        total = added(planes.at[it], outer)
        total = jnp.concatenate([total[:, :width], total[:, width:]], axis=0)
        inverse = inverse_factor(total)

        if it == 1:
            scale = jnp.sqrt(jnp.float32(cells * cell_dev))
            for r in range(parts):
                basis_out[:, r * piece : (r + 1) * piece] = (
                    jnp.dot(
                        inverse, mine[it, r] + theirs[it, r], precision=HIGH,
                        preferred_element_type=jnp.float32,
                    ) * scale
                ).astype(basis_out.dtype)

        forward(0)
        each_far(lambda source, k: far_copy(it, source, k).wait_recv())
        summed = added(sums_in.at[it], outer)
        result = jnp.dot(inverse, summed, precision=HIGH, preferred_element_type=jnp.float32)
        if it == 0:
            middle[cell] = result.astype(middle.dtype)
            each(lambda _, k: mid_copy(cell, k).start())
            each(lambda source, k: mid_copy(source, k).wait_recv())
        else:
            load_out[...] = result

    for it in range(2):
        for r in range(parts):
            pair_copy(it, r).wait_send()
        each_near(lambda _, k: gram_copy(it, spot, k).wait_send())
        each_far(lambda _, k: plane_copy(it, here, k).wait_send())
        for group in range(outer):
            each_near(lambda _, k: near_copy(it, group, spot, k).wait_send())
        each_far(lambda _, k: far_copy(it, here, k).wait_send())
    each(lambda _, k: mid_copy(cell, k).wait_send())


def local(cells, genes, tiles, tile_row, tile_col, tile_count, start_basis):
    slots, side = tiles.shape[1], tiles.shape[-1]
    width, gene_dev = start_basis.shape
    gene_blocks = gene_dev // side
    cell_dev = ROW_BLOCKS * side
    chunk = gene_dev // cells
    parts = 4
    inner = 1
    while inner * inner * 4 <= cells and cells % (inner * 2) == 0:
        inner = inner * 2
    outer = cells // inner
    places = ROW_BLOCKS * gene_blocks
    live = jnp.arange(slots) < tile_count[0, 0]
    spot = jnp.where(live, tile_row[0] * gene_blocks + tile_col[0], places)
    table = jnp.min(
        jnp.where(spot[None, :] == jnp.arange(places)[:, None], jnp.arange(slots)[None, :], slots),
        axis=1,
    ).astype(jnp.int32)
    dma = pltpu.SemaphoreType.DMA
    return pl.pallas_call(
        functools.partial(kernel, cells, inner, genes, parts),
        out_shape=(
            jax.ShapeDtypeStruct((width, cell_dev), jnp.bfloat16),
            jax.ShapeDtypeStruct((width, chunk), jnp.float32),
        ),
        in_specs=[
            pl.BlockSpec(memory_space=pltpu.SMEM),
            pl.BlockSpec(memory_space=pl.ANY),
            pl.BlockSpec(memory_space=pltpu.VMEM),
        ],
        out_specs=(
            pl.BlockSpec(memory_space=pltpu.VMEM),
            pl.BlockSpec(memory_space=pltpu.VMEM),
        ),
        scratch_shapes=[
            pltpu.VMEM((slots + 1, side, side), jnp.bfloat16),
            pltpu.VMEM((cell_dev, gene_dev), jnp.bfloat16),
            pltpu.VMEM((2, parts, width, cell_dev // parts), jnp.float32),
            pltpu.VMEM((2, parts, width, cell_dev // parts), jnp.float32),
            pltpu.VMEM((3 * width, cell_dev), jnp.bfloat16),
            pltpu.VMEM((2, inner, width // 2, 2 * width), jnp.float32),
            pltpu.VMEM((2, outer, width // 2, 2 * width), jnp.float32),
            pltpu.VMEM((2, outer, inner, width, chunk), jnp.float32),
            pltpu.VMEM((2, outer, inner, width, chunk), jnp.float32),
            pltpu.VMEM((2, outer, width, chunk), jnp.float32),
            pltpu.VMEM((2, outer, width, chunk), jnp.float32),
            pltpu.VMEM((cells, width, chunk), jnp.bfloat16),
            dma,
            dma((2, parts)), dma((2, parts)),
            dma((2, inner)), dma((2, inner)), dma((2, outer)), dma((2, outer)),
            dma((2, outer, inner)), dma((2, outer, inner)), dma((2, outer)), dma((2, outer)),
            dma((cells,)), dma((cells,)),
        ],
        compiler_params=pltpu.CompilerParams(
            collective_id=0, has_side_effects=True, vmem_limit_bytes=60 * 1024 * 1024
        ),
    )(table, tiles[0], start_basis)


def solution(mesh):
    return jax.shard_map(
        functools.partial(local, mesh.shape["cell"], mesh.shape["gene"]),
        mesh=mesh,
        in_specs=(
            P("gene", "cell", None, None),
            P("gene", "cell"),
            P("gene", "cell"),
            P("gene", "cell"),
            P(None, "gene"),
        ),
        out_specs=(P(None, "cell"), P(None, ("gene", "cell"))),
        check_vma=False,
    )
```

```python
import functools

import jax
import jax.numpy as jnp
from jax import lax
from jax.experimental import pallas as pl
from jax.experimental.pallas import tpu as pltpu
from jax.sharding import PartitionSpec as P

ROW_BLOCKS = 8
PANEL = 4
MESH = pl.DeviceIdType.MESH
HIGH = lax.Precision.HIGHEST


def split_three(value):
    high = value.astype(jnp.bfloat16)
    rest = value - high.astype(jnp.float32)
    middle = rest.astype(jnp.bfloat16)
    low = (rest - middle.astype(jnp.float32)).astype(jnp.bfloat16)
    return high, middle, low


def inverse_factor(gram):
    width = gram.shape[0]
    shape = (width, 2 * width)
    row = lax.broadcasted_iota(jnp.int32, shape, 0)
    lane = lax.broadcasted_iota(jnp.int32, shape, 1)
    both = jnp.concatenate([jnp.zeros_like(gram), gram], axis=1)
    both = jnp.where(row == lane, 1.0, both)
    pivots = jnp.ones(shape, jnp.float32)
    done = []
    start = 0
    for first in range(0, width, PANEL):
        base = first // 8 * 8
        if base > start:
            done.append((both[: base - start], pivots[: base - start]))
            both = both[base - start :]
            pivots = pivots[base - start :]
            row = row[base - start :]
            start = base
        columns = [
            jnp.broadcast_to(both[:, width + j : width + j + 1], both.shape)
            for j in range(first, first + PANEL)
        ]
        for k in range(PANEL):
            j = first + k
            at = j - start
            pivot = columns[k][at : at + 1]
            factor = jnp.where(row > j, columns[k] * (1.0 / pivot), 0.0)
            pivots = jnp.where(row == j, pivot, pivots)
            both = both - factor * both[at : at + 1]
            for m in range(k + 1, PANEL):
                columns[m] = columns[m] - factor * columns[m][at : at + 1]
    done.append((both, pivots))
    both = jnp.concatenate([piece for piece, _ in done], axis=0)
    pivots = jnp.concatenate([piece for _, piece in done], axis=0)
    return (both * lax.rsqrt(pivots))[:, :width]


def kernel(
    cells, inner, genes, parts,
    table, tiles, start, basis_out, load_out,
    held, dense, mine, theirs, stacked, grams, planes, sums_out, sums_mid, sums_own, sums_in, middle, basis,
    tile_sem, pair_send, pair_recv, gram_send, gram_recv, plane_send, plane_recv,
    near_send, near_recv, far_send, far_recv, mid_send, mid_recv,
):
    cell = lax.axis_index("cell")
    gene = lax.axis_index("gene")
    slots, side, _ = tiles.shape
    width = start.shape[0]
    cell_dev, gene_dev = dense.shape
    gene_blocks = gene_dev // side
    chunk = gene_dev // cells
    piece = cell_dev // parts
    half = width // 2
    outer = cells // inner
    here = cell // inner
    spot = lax.rem(cell, inner)
    other = lax.rem(gene + 1, genes)

    fetch = pltpu.make_async_copy(tiles, held.at[pl.ds(0, slots)], tile_sem)
    fetch.start()

    barrier = pltpu.get_barrier_semaphore()

    def greet(k, _):
        pl.semaphore_signal(
            barrier, inc=1, device_id={"cell": lax.rem(cell + k, cells)}, device_id_type=MESH
        )
        return 0

    pl.semaphore_signal(barrier, inc=1, device_id={"gene": other}, device_id_type=MESH)
    lax.fori_loop(1, cells, greet, 0)
    held[slots] = jnp.zeros((side, side), held.dtype)
    fetch.wait()

    def place(i, _):
        row = i // gene_blocks
        col = lax.rem(i, gene_blocks)
        dense[
            pl.ds(pl.multiple_of(row * side, side), side),
            pl.ds(pl.multiple_of(col * side, side), side),
        ] = held[table[i]]
        return 0

    lax.fori_loop(0, (cell_dev // side) * gene_blocks, place, 0)
    basis[...] = start[...]
    pl.semaphore_wait(barrier, cells)

    def pair_copy(it, r):
        return pltpu.make_async_remote_copy(
            src_ref=mine.at[it, r], dst_ref=theirs.at[it, r],
            send_sem=pair_send.at[it, r], recv_sem=pair_recv.at[it, r],
            device_id={"gene": other}, device_id_type=MESH,
        )

    def near(k):
        return here * inner + lax.rem(spot + k, inner)

    def far(k):
        return lax.rem(here + k, outer) * inner + spot

    def gram_copy(it, source, k):
        return pltpu.make_async_remote_copy(
            src_ref=grams.at[it, source], dst_ref=grams.at[it, source],
            send_sem=gram_send.at[it, k], recv_sem=gram_recv.at[it, source],
            device_id={"cell": near(k)}, device_id_type=MESH,
        )

    def plane_copy(it, source, k):
        return pltpu.make_async_remote_copy(
            src_ref=planes.at[it, source], dst_ref=planes.at[it, source],
            send_sem=plane_send.at[it, k], recv_sem=plane_recv.at[it, source],
            device_id={"cell": far(k)}, device_id_type=MESH,
        )

    def near_copy(it, group, source, k):
        return pltpu.make_async_remote_copy(
            src_ref=sums_out.at[it, group, lax.rem(spot + k, inner)],
            dst_ref=sums_mid.at[it, group, source],
            send_sem=near_send.at[it, group, k], recv_sem=near_recv.at[it, group, source],
            device_id={"cell": near(k)}, device_id_type=MESH,
        )

    def far_copy(it, source, k):
        return pltpu.make_async_remote_copy(
            src_ref=sums_own.at[it, lax.rem(here + k, outer)], dst_ref=sums_in.at[it, source],
            send_sem=far_send.at[it, k], recv_sem=far_recv.at[it, source],
            device_id={"cell": far(k)}, device_id_type=MESH,
        )

    def mid_copy(source, k):
        return pltpu.make_async_remote_copy(
            src_ref=middle.at[source], dst_ref=middle.at[source],
            send_sem=mid_send.at[k], recv_sem=mid_recv.at[source],
            device_id={"cell": lax.rem(cell + k, cells)}, device_id_type=MESH,
        )

    def each(act):
        def body(k, _):
            act(lax.rem(cell + cells - k, cells), k)
            return 0

        lax.fori_loop(1, cells, body, 0)

    def each_near(act):
        for k in range(1, inner):
            act(lax.rem(spot + inner - k, inner), k)

    def each_far(act):
        for k in range(1, outer):
            act(lax.rem(here + outer - k, outer), k)

    def added(ref, count):
        total = ref[0]
        for c in range(1, count):
            total = total + ref[c]
        return total

    def loop(first, last, act):
        def body(k, _):
            act(k)
            return 0

        lax.fori_loop(first, last, body, 0)

    def part(r):
        return pl.ds(pl.multiple_of(r * piece, piece), piece)

    def iteration(it):
        def score(r):
            mine[it, r] = lax.dot_general(
                basis[...], dense[part(r), :], (((1,), (1,)), ((), ())),
                preferred_element_type=jnp.float32,
            )
            pair_copy(it, r).start()

        def merge(r):
            pair_copy(it, r).wait_recv()
            high, mid, low = split_three(mine[it, r] + theirs[it, r])
            stacked[0:width, part(r)] = high
            stacked[width : 2 * width, part(r)] = mid
            stacked[2 * width : 3 * width, part(r)] = low

        loop(0, parts, score)
        loop(0, parts, merge)

        whole = stacked[...]
        cross = lax.dot_general(
            whole, whole, (((1,), (1,)), ((), ())), preferred_element_type=jnp.float32
        )
        cross = cross[:width] + cross[width : 2 * width] + cross[2 * width :]
        gram = cross[:, :width] + cross[:, width : 2 * width] + cross[:, 2 * width :]
        grams[it, spot] = jnp.concatenate([gram[:half], gram[half:]], axis=1)
        each_near(lambda _, k: gram_copy(it, spot, k).start())

        def product(columns):
            pair = jnp.dot(
                stacked[0 : 2 * width, :], columns, preferred_element_type=jnp.float32
            )
            return pair[:width] + pair[width:]

        span = inner * chunk

        def multiply(k):
            group = lax.rem(here + k, outer)
            if span % 128 == 0:
                wide = product(dense[:, pl.ds(pl.multiple_of(group * span, 128), span)])
                for c in range(inner):
                    sums_out[it, group, c] = wide[:, c * chunk : (c + 1) * chunk]
            each_near(lambda _, k: near_copy(it, group, spot, k).start())

        def forward(k):
            group = lax.rem(here + k, outer)
            each_near(lambda source, k: near_copy(it, group, source, k).wait_recv())
            total = sums_out[it, group, spot]
            for c in range(1, inner):
                total = total + sums_mid[it, group, lax.rem(spot + c, inner)]
            if isinstance(k, int):
                sums_in[it, here] = total
            else:
                sums_own[it, group] = total
                far_copy(it, here, k).start()

        if span % 128 != 0:
            for b in range(gene_blocks):
                wide = product(dense[:, b * side : (b + 1) * side])
                for c in range(side // chunk):
                    at = b * (side // chunk) + c
                    sums_out[it, at // inner, at % inner] = wide[:, c * chunk : (c + 1) * chunk]
        multiply(1)
        each_near(lambda source, k: gram_copy(it, source, k).wait_recv())
        planes[it, here] = added(grams.at[it], inner)
        each_far(lambda _, k: plane_copy(it, here, k).start())
        loop(2, outer + 1, multiply)
        loop(1, outer, forward)
        each_far(lambda source, k: plane_copy(it, source, k).wait_recv())
        total = added(planes.at[it], outer)
        total = jnp.concatenate([total[:, :width], total[:, width:]], axis=0)
        inverse = inverse_factor(total)

        @pl.when(it == 1)
        def _():
            scale = jnp.sqrt(jnp.float32(cells * cell_dev))

            def finish(r):
                basis_out[:, part(r)] = (
                    jnp.dot(
                        inverse, mine[it, r] + theirs[it, r], precision=HIGH,
                        preferred_element_type=jnp.float32,
                    ) * scale
                ).astype(basis_out.dtype)

            loop(0, parts, finish)

        forward(0)
        each_far(lambda source, k: far_copy(it, source, k).wait_recv())
        summed = added(sums_in.at[it], outer)
        result = jnp.dot(inverse, summed, precision=HIGH, preferred_element_type=jnp.float32)

        @pl.when(it == 0)
        def _():
            middle[cell] = result.astype(middle.dtype)
            each(lambda _, k: mid_copy(cell, k).start())
            each(lambda source, k: mid_copy(source, k).wait_recv())
            basis[...] = jnp.concatenate([middle[c] for c in range(cells)], axis=1)

        @pl.when(it == 1)
        def _():
            load_out[...] = result

    loop(0, 2, iteration)

    def drain(it):
        loop(0, parts, lambda r: pair_copy(it, r).wait_send())
        each_near(lambda _, k: gram_copy(it, spot, k).wait_send())
        each_far(lambda _, k: plane_copy(it, here, k).wait_send())
        loop(0, outer, lambda group: each_near(lambda _, k: near_copy(it, group, spot, k).wait_send()))
        each_far(lambda _, k: far_copy(it, here, k).wait_send())

    loop(0, 2, drain)
    each(lambda _, k: mid_copy(cell, k).wait_send())


def local(cells, genes, tiles, tile_row, tile_col, tile_count, start_basis):
    slots, side = tiles.shape[1], tiles.shape[-1]
    width, gene_dev = start_basis.shape
    gene_blocks = gene_dev // side
    cell_dev = ROW_BLOCKS * side
    chunk = gene_dev // cells
    parts = 4
    inner = 1
    while inner * inner * 4 <= cells and cells % (inner * 2) == 0:
        inner = inner * 2
    outer = cells // inner
    places = ROW_BLOCKS * gene_blocks
    live = jnp.arange(slots) < tile_count[0, 0]
    spot = jnp.where(live, tile_row[0] * gene_blocks + tile_col[0], places)
    table = jnp.min(
        jnp.where(spot[None, :] == jnp.arange(places)[:, None], jnp.arange(slots)[None, :], slots),
        axis=1,
    ).astype(jnp.int32)
    dma = pltpu.SemaphoreType.DMA
    return pl.pallas_call(
        functools.partial(kernel, cells, inner, genes, parts),
        out_shape=(
            jax.ShapeDtypeStruct((width, cell_dev), jnp.bfloat16),
            jax.ShapeDtypeStruct((width, chunk), jnp.float32),
        ),
        in_specs=[
            pl.BlockSpec(memory_space=pltpu.SMEM),
            pl.BlockSpec(memory_space=pl.ANY),
            pl.BlockSpec(memory_space=pltpu.VMEM),
        ],
        out_specs=(
            pl.BlockSpec(memory_space=pltpu.VMEM),
            pl.BlockSpec(memory_space=pltpu.VMEM),
        ),
        scratch_shapes=[
            pltpu.VMEM((slots + 1, side, side), jnp.bfloat16),
            pltpu.VMEM((cell_dev, gene_dev), jnp.bfloat16),
            pltpu.VMEM((2, parts, width, cell_dev // parts), jnp.float32),
            pltpu.VMEM((2, parts, width, cell_dev // parts), jnp.float32),
            pltpu.VMEM((3 * width, cell_dev), jnp.bfloat16),
            pltpu.VMEM((2, inner, width // 2, 2 * width), jnp.float32),
            pltpu.VMEM((2, outer, width // 2, 2 * width), jnp.float32),
            pltpu.VMEM((2, outer, inner, width, chunk), jnp.float32),
            pltpu.VMEM((2, outer, inner, width, chunk), jnp.float32),
            pltpu.VMEM((2, outer, width, chunk), jnp.float32),
            pltpu.VMEM((2, outer, width, chunk), jnp.float32),
            pltpu.VMEM((cells, width, chunk), jnp.bfloat16),
            pltpu.VMEM((width, gene_dev), jnp.bfloat16),
            dma,
            dma((2, parts)), dma((2, parts)),
            dma((2, inner)), dma((2, inner)), dma((2, outer)), dma((2, outer)),
            dma((2, outer, inner)), dma((2, outer, inner)), dma((2, outer)), dma((2, outer)),
            dma((cells,)), dma((cells,)),
        ],
        compiler_params=pltpu.CompilerParams(
            collective_id=0, has_side_effects=True, vmem_limit_bytes=60 * 1024 * 1024
        ),
    )(table, tiles[0], start_basis)


def solution(mesh):
    return jax.shard_map(
        functools.partial(local, mesh.shape["cell"], mesh.shape["gene"]),
        mesh=mesh,
        in_specs=(
            P("gene", "cell", None, None),
            P("gene", "cell"),
            P("gene", "cell"),
            P("gene", "cell"),
            P(None, "gene"),
        ),
        out_specs=(P(None, "cell"), P(None, ("gene", "cell"))),
        check_vma=False,
    )
```
